128 devices in a mesh: groups: 4 (over x, y), tensor: 32 (over z, core).
Axes of the slice: x: 2, y: 2, z: 16, core: 2. Of those that a mesh axis runs over, the one named last changes fastest.
The devices are a block of a 8x8x16 slice.
Arguments:
- hidden_in: bfloat16 [1024, 8192], P(('groups', 'tensor')), parts along dimension 0, may hold values from -6 to 6
- norm_gain: bfloat16 [8192], replicated, may hold values from 0.25 to 1.75
- w_query: bfloat16 [8192, 64, 128], P(None, 'tensor'), may hold values from -0.0625 to 0.0625
- w_kv: bfloat16 [8192, 8, 2, 128], P('tensor'), may hold values from -0.5 to 0.5
- w_out: bfloat16 [64, 128, 8192], P('tensor'), may hold values from -0.0625 to 0.0625
- prefix_keys: bfloat16 [128, 6, 2048, 128], P(('groups', 'tensor')), parts along dimension 0, may hold values from -1000 to 1000
- prefix_values: bfloat16 [128, 6, 2048, 128], P(('groups', 'tensor')), parts along dimension 0, may hold values from -6 to 6
- suffix_keys: bfloat16 [128, 126, 256, 128], P(('groups', 'tensor')), parts along dimension 0, may hold values from -10 to 10
- suffix_values: bfloat16 [128, 126, 256, 128], P(('groups', 'tensor')), parts along dimension 0, may hold values from -6 to 6
- row_counts: int32 [96], P('groups'), parts along dimension 0, may hold values from 1 to 21, 256 in all
- suffix_lengths: int32 [1024], P('groups'), parts along dimension 0, may hold values from 1 to 256
Outputs:
- layer_out: bfloat16 [1024, 8192], P(('groups', 'tensor')), parts along dimension 0
The draws below stay inside these ranges and needn't reach their ends.
There are 4 independent parts, one for each index of `groups`. The reference program is written for one: setup_inputs(seed, part) draws one part's arguments, and reference() takes and returns one part's arrays. A program takes and returns all parts, laid end to end along the dimension named above; an argument that names none is the same for every part. Nothing has to cross between parts.
Inputs may be any that keep to these rules, and one draw needn't show every extreme that they name: `row_counts`: critique rows are stored prompt by prompt: the rows of prompt p follow those of prompts 0 to p - 1. The counts sum to 256, and some prompt has exactly 21 rows.
All inputs are finite; a program needn't handle non-finite values.
Results may differ from the reference program's by a relative error of at most 0.023.
The reference program's roundings to bfloat16 on the way count: a program that leaves them out, or rounds other values in their place, can miss the bound.
Values may be sent and summed in bfloat16 or wider, within the bound.
A program may use at most 128 MiB of HBM per device.

```python
import math
import jax
import jax.numpy as jnp
import numpy as np
from jax import lax

D = 8192
KVH = 8
HQG = 8
HD = 128
PREFIX = 2048
SMAX = 256
PROM_DEV = 6
PCAP = 21
SLOTS = 126
PROMPTS = 24
ROWS = 256
OWNERS = 32
N_TENSOR = 32


def draw_prefix_keys(key, part):
    base_key = jax.random.fold_in(jax.random.fold_in(key, 11), 0)
    values = jnp.clip(jax.random.normal(base_key, (OWNERS, PROM_DEV, PREFIX, HD), jnp.float32), -4.0, 4.0) * 2.5
    return values.astype(jnp.bfloat16)


def set_ends(result, stream_key, least, top_value):
    extent = result.shape
    index_at = [jax.random.randint(jax.random.fold_in(stream_key, axis), (), 0, extent[axis]) for axis in range(len(extent))]
    result = result.at[tuple(index_at)].set(least)
    longest = extent.index(max(extent))
    index_at[longest] = (index_at[longest] + 1) % extent[longest]
    return result.at[tuple(index_at)].set(top_value)


def level_of(key, shape, cuts, low, largest):
    def one(position, shards_of):
        draws = jax.random.uniform(jax.random.fold_in(jax.random.fold_in(key, 6), position), (shards_of,), jnp.float32, low / len(cuts), largest / len(cuts))
        return jnp.repeat(jnp.exp(draws), shape[position] // shards_of).reshape((-1,) + (1,) * (len(shape) - position - 1))

    level = one(*cuts[0])
    for cut in cuts[1:]:
        level = level * one(*cut)
    return level


def profile(amount, total, most, skew):
    loads = [(1 << 20) // math.isqrt(rank ** skew) + 1 for rank in range(2, amount + 1)]
    surplus, holding = total - most - (amount - 1), [1] * (amount - 1)
    while surplus > 0:
        candidates = [i for i in range(amount - 1) if holding[i] < most]
        pool, remaining = sum([loads[i] for i in candidates]), surplus
        for i in candidates:
            addition = min(most - holding[i], max(1, remaining * loads[i] // pool), surplus)
            holding[i] = holding[i] + addition
            surplus = surplus - addition
    return np.array([most] + holding)


def uneven(stream_key, count, total, reach, skew):
    if count == 2:
        one = jax.random.randint(stream_key, (), max(1, total - reach), min(reach, total - 1) + 1)
        return jnp.stack([one, total - one])
    lengths = jnp.asarray(profile(count, total, reach, skew), jnp.int32)
    pairs = (count - 1) // 2
    giver, taker = lengths[1:1 + 2 * pairs:2], lengths[2:2 + 2 * pairs:2]
    margin = jnp.minimum(giver - 1, reach - taker)
    shifted = jax.random.randint(jax.random.fold_in(stream_key, 1), (pairs,), 0, 1 << 20) % (margin + 1)
    lengths = lengths.at[1:1 + 2 * pairs:2].set(giver - shifted).at[2:2 + 2 * pairs:2].set(taker + shifted)
    return lengths[jax.random.permutation(jax.random.fold_in(stream_key, 2), count)]


def normal_values(own_key, shape, scale, reach, cuts=(), kind=jnp.bfloat16):
    loudness = level_of(own_key, shape, cuts, -0.22, 0.18) if cuts else 1.0
    entries = jax.random.normal(own_key, shape, jnp.float32) * scale * loudness
    return jnp.minimum(jnp.maximum(entries, -reach), reach).astype(kind)


def setup_inputs(seed: int = 0, part: int = 0) -> dict:
    key_list = jax.random.split(jax.random.key(seed), 12)
    own_keys = jax.random.split(jax.random.fold_in(key_list[11], part), 12)
    return {
        "hidden_in": normal_values(own_keys[0], (ROWS, D), 1.0, 6.0, ((0, 32),)),
        "norm_gain": jnp.clip(1.0 + 0.15 * jax.random.normal(key_list[1], (D,), jnp.float32), 0.25, 1.75).astype(jnp.bfloat16),
        "w_query": normal_values(key_list[2], (D, KVH * HQG, HD), D ** -0.5, 0.0625, ((1, 32),)),
        "w_kv": normal_values(key_list[3], (D, KVH, 2, HD), (D // 64) ** -0.5, 0.5, ((0, 32),)),
        "w_out": normal_values(key_list[4], (KVH * HQG, HD, D), (KVH * HQG * HD) ** -0.5, 0.0625, ((0, 32),)),
        "prefix_keys": draw_prefix_keys(jax.random.fold_in(jax.random.fold_in(key_list[11], part), 71), part),
        "prefix_values": normal_values(own_keys[6], (OWNERS, PROM_DEV, PREFIX, HD), 1.0, 6.0, ((0, 32),)),
        "suffix_keys": normal_values(own_keys[7], (OWNERS, SLOTS, SMAX, HD), 2.5, 10.0, ((0, 32),)),
        "suffix_values": normal_values(own_keys[8], (OWNERS, SLOTS, SMAX, HD), 1.0, 6.0, ((0, 32),)),
        "row_counts": uneven(own_keys[9], PROMPTS, ROWS, PCAP, 2).astype(jnp.int32),
        "suffix_lengths": set_ends(jax.random.randint(own_keys[10], (ROWS,), 1, SMAX + 1), jax.random.fold_in(own_keys[10], 1), 1, SMAX).astype(jnp.int32),
    }


def rotate(vector, angle):
    half_size = vector.shape[-1] // 2
    front_half = vector[..., :half_size]
    back_half = vector[..., half_size:]
    cosines = jnp.cos(angle)
    sine_terms = jnp.sin(angle)
    return jnp.concatenate([front_half * cosines - back_half * sine_terms, back_half * cosines + front_half * sine_terms], axis=-1)

def rotation_angles(positions):
    frequency = 500000.0 ** (-(2.0 * jnp.arange(HD // 2, dtype=jnp.float32)) / HD)
    return positions.astype(jnp.float32)[:, None] * frequency[None, :]

def reference(hidden_in, norm_gain, w_query, w_kv, w_out, prefix_keys, prefix_values, suffix_keys, suffix_values, row_counts, suffix_lengths):
    rows_all = hidden_in.shape[0]
    widened = hidden_in.astype(jnp.float32)
    inverse_norm = lax.rsqrt(lax.optimization_barrier(jnp.mean(widened * widened, axis=1, keepdims=True)) + 1e-05)
    normed = (widened * inverse_norm * norm_gain.astype(jnp.float32)[None, :]).astype(jnp.bfloat16)
    query_raw = jnp.dot(normed, w_query.reshape(D, KVH * HQG * HD), preferred_element_type=jnp.float32)
    query_raw = query_raw.astype(jnp.bfloat16).reshape(rows_all, KVH, HQG, HD)
    kv_raw = jnp.dot(normed, w_kv.reshape(D, KVH * 2 * HD), preferred_element_type=jnp.float32)
    kv_raw = kv_raw.astype(jnp.bfloat16).reshape(rows_all, KVH, 2, HD)
    row_ends = jnp.cumsum(row_counts).astype(jnp.int32)
    row_starts = (row_ends - row_counts).astype(jnp.int32)
    row_index = jnp.arange(rows_all, dtype=jnp.int32)
    prompt_of = lax.optimization_barrier(jnp.sum((row_index[:, None] >= row_ends[None, :]).astype(jnp.int32), axis=1)).astype(jnp.int32)
    offsets = (row_index - row_starts[prompt_of]).astype(jnp.int32)
    rotation = rotation_angles(PREFIX + suffix_lengths)
    queries = rotate(query_raw.astype(jnp.float32), rotation[:, None, None, :]).astype(jnp.bfloat16)
    new_keys = rotate(kv_raw[:, :, 0].astype(jnp.float32), rotation[:, None, :]).astype(jnp.bfloat16)
    new_values = kv_raw[:, :, 1]
    head_index = jnp.arange(KVH, dtype=jnp.int32)
    scaling = 1.0 / HD ** 0.5

    def single_row(inputs):
        query_row, key_row, value_row, prompt, offset_row, length = inputs
        owners = prompt // PROM_DEV * KVH + head_index
        local_prompt = prompt % PROM_DEV
        slot_index = local_prompt * PCAP + offset_row
        past_keys = prefix_keys[owners, local_prompt].astype(jnp.float32)
        past_values = prefix_values[owners, local_prompt].astype(jnp.float32)
        tail_keys = suffix_keys[owners, slot_index].astype(jnp.float32)
        tail_values = suffix_values[owners, slot_index].astype(jnp.float32)
        query_wide = query_row.astype(jnp.float32)
        prefix_scores = jnp.einsum('hjd,htd->hjt', query_wide, past_keys) * scaling
        suffix_scores = jnp.einsum('hjd,htd->hjt', query_wide, tail_keys) * scaling
        visible = jnp.arange(SMAX) < length
        suffix_scores = jnp.where(visible[None, None, :], suffix_scores, -jnp.inf)
        self_score = jnp.einsum('hjd,hd->hj', query_wide, key_row.astype(jnp.float32)) * scaling
        highest = jnp.maximum(lax.optimization_barrier(jnp.max(prefix_scores, axis=2)), jnp.maximum(lax.optimization_barrier(jnp.max(suffix_scores, axis=2)), self_score))
        prefix_exp = jnp.exp(prefix_scores - highest[..., None])
        suffix_exp = jnp.exp(suffix_scores - highest[..., None])
        self_exp = jnp.exp(self_score - highest)
        totals = lax.optimization_barrier(jnp.sum(prefix_exp, axis=2)) + lax.optimization_barrier(jnp.sum(suffix_exp, axis=2)) + self_exp
        prefix_weights = lax.optimization_barrier((prefix_exp / totals[..., None]).astype(jnp.bfloat16)).astype(jnp.float32)
        suffix_weights = lax.optimization_barrier((suffix_exp / totals[..., None]).astype(jnp.bfloat16)).astype(jnp.float32)
        self_weight = lax.optimization_barrier((self_exp / totals).astype(jnp.bfloat16)).astype(jnp.float32)
        combined = jnp.einsum('hjt,htd->hjd', prefix_weights, past_values)
        combined = combined + jnp.einsum('hjt,htd->hjd', suffix_weights, tail_values)
        combined = combined + self_weight[..., None] * value_row.astype(jnp.float32)[:, None, :]
        return combined.astype(jnp.bfloat16)
    attended = lax.map(single_row, (queries, new_keys, new_values, prompt_of, offsets, suffix_lengths))
    head_share = KVH * HQG // N_TENSOR
    attended_blocks = attended.reshape(rows_all, N_TENSOR, head_share * HD)
    weight_blocks = w_out.reshape(N_TENSOR, head_share * HD, D)

    def add_block(total, index):
        term = jnp.dot(attended_blocks[:, index], weight_blocks[index], preferred_element_type=jnp.float32)
        term = lax.optimization_barrier(term.astype(jnp.bfloat16)).astype(jnp.float32)
        return (total + term, None)
    summed, unused = lax.scan(add_block, jnp.zeros((rows_all, D), jnp.float32), jnp.arange(N_TENSOR, dtype=jnp.int32))
    return (widened + summed).astype(jnp.bfloat16)
```

```python
import functools
import math

import jax
import jax.numpy as jnp
from jax import lax
from jax.experimental import pallas as pl
from jax.experimental.pallas import tpu as pltpu
from jax.sharding import Mesh
from jax.sharding import PartitionSpec as P

HD = 128
PREFIX = 2048
PCAP = 21
PAD = 128
TENSOR = ("tensor_0", "tensor_1")
GROUPS_TENSOR = ("groups", "tensor_0", "tensor_1")
MESH = pl.DeviceIdType.MESH
KVT = jnp.float32
XCH = 4
RCH = 8
F32 = jnp.float32
BF16 = jnp.bfloat16


def at(z, c):
    return {"tensor_0": z, "tensor_1": c}


def remote(src, dst, send, recv, z, c):
    return pltpu.make_async_remote_copy(
        src_ref=src, dst_ref=dst, send_sem=send, recv_sem=recv, device_id=at(z, c), device_id_type=MESH
    )


def project_kernel(
    chips, hidden, gain, wq_hbm, wkv_hbm, cosf, sinf, slots, q_out, kv_out,
    x, wq, wkv, kvs, kvr, qs, kvh, kvl,
    wq_sem, wkv_sem, wkvs_sem, wkvr_sem, xs, xr, ps, pr, ks, kr, qss, qrs, qls, as_, ar, al,
):
    z = lax.axis_index("tensor_0")
    c = lax.axis_index("tensor_1")
    devices = 2 * chips
    half = chips // 2
    me = 2 * z + c
    right = lax.rem(z + 1, chips)
    left = lax.rem(z + chips - 1, chips)
    slab = wkv_hbm.shape[0]
    width = x.shape[2] // XCH
    barrier = pltpu.get_barrier_semaphore()

    def greet(n, carry):
        @pl.when(n != me)
        def _():
            pl.semaphore_signal(barrier, inc=1, device_id=at(n // 2, lax.rem(n, 2)), device_id_type=MESH)

        return carry

    lax.fori_loop(0, devices, greet, 0)
    load_wq = pltpu.make_async_copy(wq_hbm, wq, wq_sem)
    load_wq.start()
    own_rows = pl.ds(pl.multiple_of(c * slab, slab), slab)
    load_wkv = pltpu.make_async_copy(wkv_hbm, wkv.at[own_rows, :], wkv_sem)
    load_wkv.start()

    wide = hidden[...].astype(F32)
    inverse = lax.rsqrt(jnp.mean(wide * wide, axis=1, keepdims=True) + 1e-05)
    x[me] = (wide * inverse * gain[...].astype(F32)).astype(BF16)
    kvs[1, 0] = jnp.zeros(kvs.shape[2:], kvs.dtype)

    pl.semaphore_wait(barrier, devices - 1)

    send_wkv = remote(wkv_hbm, wkv.at[own_rows, :], wkvs_sem, wkvr_sem, z, 1 - c)
    send_wkv.start()

    def row_copy(way, step, j, shard):
        piece = x.at[shard, :, pl.ds(j * width, width)]
        return remote(piece, piece, xs.at[way, step, j], xr.at[way, step, j], right if way == 0 else left, c)

    def part_copy(way, step, shard):
        return remote(x.at[shard], x.at[shard], ps.at[way, step], pr.at[way, step], z, 1 - c)

    def kv_copy(way, step):
        return remote(kvs.at[way, step], kvr.at[way, step], ks.at[way, step], kr.at[way, step], right if way == 0 else left, c)

    for j in range(XCH):
        row_copy(0, 0, j, me).start()
        row_copy(1, 0, j, me).start()
    part_copy(0, 0, me).start()
    kv_copy(1, 0).start()
    feats = pl.ds(pl.multiple_of(z * 2 * slab, 2 * slab), 2 * slab)

    load_wkv.wait()
    send_wkv.wait()
    own = jnp.dot(x[me, :, feats], wkv[...], preferred_element_type=F32)
    kvs[0, 0] = own.astype(kvs.dtype)
    kv_copy(0, 0).start()

    def hop(s, carry):
        cw = 2 * lax.rem(z - s + chips, chips) + c
        ccw = 2 * lax.rem(z + s, chips) + c
        for j in range(XCH):
            row_copy(0, s - 1, j, cw).wait_recv()
            row_copy(0, s, j, cw).start()
            row_copy(1, s - 1, j, ccw).wait_recv()

            @pl.when(s < half - 1)
            def _():
                row_copy(1, s, j, ccw).start()

        part_copy(0, s, cw).start()
        part_copy(1, s, ccw).start()
        both = jnp.concatenate([x[cw, :, feats].astype(F32), x[ccw, :, feats].astype(F32)], axis=0).astype(BF16)
        part = jnp.dot(both, wkv[...], preferred_element_type=F32)
        kv_copy(0, s - 1).wait_recv()
        kvs[0, s] = (part[:8] + kvr[0, s - 1].astype(F32)).astype(kvs.dtype)
        kv_copy(0, s).start()
        kv_copy(1, s - 1).wait_recv()
        kvs[1, s] = (part[8:] + kvr[1, s - 1].astype(F32)).astype(kvs.dtype)
        kv_copy(1, s).start()
        return carry

    lax.fori_loop(1, half, hop, 0)
    far = 2 * lax.rem(z + half, chips) + c
    for j in range(XCH):
        row_copy(0, half - 1, j, far).wait_recv()
    part_copy(0, half, far).start()
    own = jnp.dot(x[far, :, feats], wkv[...], preferred_element_type=F32)
    kv_copy(0, half - 1).wait_recv()
    kv_copy(1, half - 1).wait_recv()
    kv_raw = (own + kvr[0, half - 1].astype(F32) + kvr[1, half - 1].astype(F32)).astype(BF16).astype(F32)
    far_rows = pl.ds(pl.multiple_of(far * 8, 8), 8)
    cos8 = cosf[far_rows, :]
    sin8 = sinf[far_rows, :]
    heads = kvh.shape[0]
    for h in range(heads):
        key = kv_raw[:, h * 2 * HD : h * 2 * HD + HD]
        value = kv_raw[:, h * 2 * HD + HD : (h + 1) * 2 * HD]
        kvh[h, :, :HD] = (key * cos8 + pltpu.roll(key, HD // 2, 1) * sin8).astype(BF16)
        kvh[h, :, HD:] = value.astype(BF16)

    def kv_send(n):
        return remote(kvh.at[lax.rem(n, heads)], kvl.at[far], as_.at[n], ar.at[far], n // 2, lax.rem(n, 2))

    kv_self = pltpu.make_async_copy(kvh.at[lax.rem(me, heads)], kvl.at[far], al)

    def kv_out_loop(n, carry):
        @pl.when(n != me)
        def _():
            kv_send(n).start()

        return carry

    lax.fori_loop(0, devices, kv_out_loop, 0)
    kv_self.start()

    part_copy(0, 0, 2 * z + 1 - c).wait_recv()

    def part_wait(s, carry):
        part_copy(0, s, me).wait_recv()
        part_copy(1, s, me).wait_recv()
        return carry

    lax.fori_loop(1, half, part_wait, 0)
    part_copy(0, half, me).wait_recv()
    load_wq.wait()
    depth = 1024
    rows = devices * 8

    def q_step(k, acc):
        piece = pl.ds(pl.multiple_of(k * depth, depth), depth)
        xk = x[:, :, piece].astype(F32).reshape(rows, depth).astype(BF16)
        return acc + jnp.dot(xk, wq[piece, :], preferred_element_type=F32)

    acc = lax.fori_loop(0, x.shape[2] // depth, q_step, jnp.zeros((rows, 2 * HD), F32))
    q_raw = acc.astype(BF16).astype(F32)
    roped = []
    for j in range(2):
        v = q_raw[:, j * HD : (j + 1) * HD]
        roped.append((v * cosf[...] + pltpu.roll(v, HD // 2, 1) * sinf[...]).astype(BF16))
    roped = jnp.concatenate(roped, axis=1)
    groups = qs.shape[0]
    hit = lax.broadcasted_iota(jnp.int32, (groups * PAD, rows), 1) == slots[...]
    pick = jnp.where(hit, 1.0, 0.0).astype(BF16)
    picked = jnp.dot(pick, roped, preferred_element_type=F32).astype(BF16)
    block = 2 * lax.rem(z, 2) + c
    my_head = lax.rem(me, heads)

    def q_send(g):
        owner = heads * g + z // 2
        return remote(qs.at[g], q_out.at[block], qss.at[g], qrs.at[block], owner // 2, lax.rem(owner, 2))

    def q_local(g):
        return pltpu.make_async_copy(qs.at[g], q_out.at[block], qls)

    for g in range(groups):
        qs[g] = picked[g * PAD : (g + 1) * PAD]
        owner = heads * g + z // 2

        @pl.when(owner != me)
        def _():
            q_send(g).start()

        @pl.when(owner == me)
        def _():
            q_local(g).start()

    def kv_in_loop(n, carry):
        @pl.when(n != far)
        def _():
            remote(kvh.at[0], kvl.at[n], as_.at[0], ar.at[n], z, 1 - c).wait_recv()

        return carry

    lax.fori_loop(0, devices, kv_in_loop, 0)
    kv_self.wait()
    mine = slots[pl.ds(pl.multiple_of(z // (heads // 2) * PAD, PAD), PAD), :]
    hit = lax.broadcasted_iota(jnp.int32, (PAD, rows), 1) == mine
    pick = jnp.where(hit, 1.0, 0.0).astype(BF16)
    table = kvl[...].astype(F32).reshape(rows, 2 * HD).astype(BF16)
    kv_out[...] = jnp.dot(pick, table, preferred_element_type=F32).astype(BF16)

    for b in range(groups):
        source = groups * my_head + b

        @pl.when(source != me)
        def _():
            remote(qs.at[0], q_out.at[b], qss.at[0], qrs.at[b], z, 1 - c).wait_recv()

    for g in range(groups):
        owner = heads * g + z // 2

        @pl.when(owner == me)
        def _():
            q_local(g).wait()

        @pl.when(owner != me)
        def _():
            q_send(g).wait_send()

    for j in range(XCH):
        row_copy(0, 0, j, me).wait_send()
        row_copy(1, 0, j, me).wait_send()
    part_copy(0, 0, me).wait_send()
    kv_copy(0, 0).wait_send()
    kv_copy(1, 0).wait_send()

    def drain(s, carry):
        for j in range(XCH):
            row_copy(0, s, j, me).wait_send()

            @pl.when(s < half - 1)
            def _():
                row_copy(1, s, j, me).wait_send()

        part_copy(0, s, me).wait_send()
        part_copy(1, s, me).wait_send()
        kv_copy(0, s).wait_send()
        kv_copy(1, s).wait_send()
        return carry

    lax.fori_loop(1, half, drain, 0)
    part_copy(0, half, me).wait_send()

    def kv_drain(n, carry):
        @pl.when(n != me)
        def _():
            kv_send(n).wait_send()

        return carry

    lax.fori_loop(0, devices, kv_drain, 0)


def attend_kernel(lens, q, kv, pk, pv, sk, sv, out, qf, kf, vf, ss, pvacc, att):
    i = pl.program_id(0)
    scaling = 1.0 / math.sqrt(HD)
    per = qf.shape[0] // PAD
    rows = PCAP * per

    @pl.when(i == 0)
    def _():
        key = kv[:, :HD].astype(F32)
        value = kv[:, HD:].astype(F32)
        for j in range(per):
            qf[pl.ds(j, PAD, stride=per), :] = q[j // 2, :, (j % 2) * HD : (j % 2 + 1) * HD].astype(F32)
            kf[pl.ds(j, PAD, stride=per), :] = key
            vf[pl.ds(j, PAD, stride=per), :] = value
        att[...] = jnp.zeros_like(att)

    mine = pl.ds(pl.multiple_of(i * rows, 8), rows)
    qi = qf[mine, :]
    qb = qi.astype(BF16)
    contract = (((1,), (1,)), ((), ()))
    ps = lax.dot_general(qb, pk[0], contract, preferred_element_type=F32) * scaling
    for r in range(PCAP):
        q8 = qf[pl.ds(pl.multiple_of(i * rows + r * per, 8), per), :].astype(BF16)
        s8 = lax.dot_general(q8, sk[r], contract, preferred_element_type=F32) * scaling
        seen = lax.broadcasted_iota(jnp.int32, s8.shape, 1) < lens[i * PCAP + r]
        ss[r * per : (r + 1) * per, :] = jnp.where(seen, s8, -jnp.inf)
    self_score = jnp.sum(qi * kf[mine, :], axis=1, keepdims=True) * scaling
    sfx = ss[...]
    top = jnp.maximum(jnp.max(ps, axis=1, keepdims=True), jnp.maximum(jnp.max(sfx, axis=1, keepdims=True), self_score))
    pe = jnp.exp(ps - top)
    se = jnp.exp(sfx - top)
    own = jnp.exp(self_score - top)
    total = jnp.sum(pe, axis=1, keepdims=True) + jnp.sum(se, axis=1, keepdims=True) + own
    acc = jnp.dot(pe.astype(BF16), pv[0], preferred_element_type=F32)
    ss[...] = se
    for r in range(PCAP):
        w8 = ss[r * per : (r + 1) * per, :].astype(BF16)
        pvacc[r * per : (r + 1) * per, :] = jnp.dot(w8, sv[r], preferred_element_type=F32)
    acc = acc + pvacc[...] + own * vf[mine, :]
    att[mine, :] = acc / total

    @pl.when(i == pl.num_programs(0) - 1)
    def _():
        for j in range(per):
            out[j // 2, :, (j % 2) * HD : (j % 2 + 1) * HD] = att[pl.ds(j, PAD, stride=per), :].astype(BF16)


def output_kernel(
    chips, hidden, att, wo_hbm, slots, out,
    a, w2, x2, p, rs, rr,
    wo_sem, wos, wor, ass, ars, als, xss, xrs, ss, sr,
):
    z = lax.axis_index("tensor_0")
    c = lax.axis_index("tensor_1")
    devices = 2 * chips
    half = chips // 2
    me = 2 * z + c
    right = lax.rem(z + 1, chips)
    left = lax.rem(z + chips - 1, chips)
    blocks = att.shape[0]
    heads = devices // blocks
    groups = blocks
    my_group = me // heads
    my_head = lax.rem(me, heads)
    width = hidden.shape[1] // RCH
    rows = devices * 8
    barrier = pltpu.get_barrier_semaphore()

    def greet(n):
        pl.semaphore_signal(barrier, inc=1, device_id=at(n // 2, lax.rem(n, 2)), device_id_type=MESH)

    greet(2 * right + c)
    greet(2 * left + c)
    greet(2 * z + 1 - c)
    for g in range(groups):
        source = heads * g + me // blocks

        @pl.when(source != me)
        def _():
            greet(source)

    load = pltpu.make_async_copy(wo_hbm, w2.at[c], wo_sem)
    load.start()
    kept = jnp.where(me // blocks == my_head, 1, 0)
    pl.semaphore_wait(barrier, 3 + blocks - kept)

    def a_send(b):
        dest = blocks * my_head + b
        return remote(att.at[b], a.at[my_group], ass.at[b], ars.at[my_group], dest // 2, lax.rem(dest, 2))

    def a_local(b):
        return pltpu.make_async_copy(att.at[b], a.at[my_group], als)

    for b in range(blocks):
        dest = blocks * my_head + b

        @pl.when(dest != me)
        def _():
            a_send(b).start()

        @pl.when(dest == me)
        def _():
            a_local(b).start()

    send_w = remote(wo_hbm, w2.at[c], wos, wor, z, 1 - c)
    send_w.start()

    for g in range(groups):
        source = heads * g + me // blocks

        @pl.when(source != me)
        def _():
            remote(att.at[0], a.at[g], ass.at[0], ars.at[g], z, 1 - c).wait_recv()

    for b in range(blocks):
        dest = blocks * my_head + b

        @pl.when(dest == me)
        def _():
            a_local(b).wait()

        @pl.when(dest != me)
        def _():
            a_send(b).wait_send()

    order = lax.broadcasted_iota(jnp.int32, (rows, groups * PAD), 0)
    wanted = (lax.rem(order, rows // 2) // 8 * 2 + order // (rows // 2)) * 8 + lax.rem(order, 8)
    pick = jnp.where(wanted == slots[...], 1.0, 0.0).astype(BF16)
    table = a[...].reshape(groups * PAD, 2 * HD)
    picked = jnp.dot(pick, table, preferred_element_type=F32).astype(BF16)
    x2[0, 0] = picked[: rows // 2]
    x2[0, 1] = picked[rows // 2 :]
    swap = remote(x2.at[0, 1 - c], x2.at[1, 0], xss, xrs, z, 1 - c)
    swap.start()
    load.wait()
    send_w.wait()
    swap.wait()

    def ring(way, step, j):
        return remote(rs.at[way, step, j], rr.at[way, step, j], ss.at[way, step, j], sr.at[way, step, j], right if way == 0 else left, c)

    def block_of(chip, cols):
        return p[pl.ds(pl.multiple_of(chip * 8, 8), 8), cols]

    far = lax.rem(z + half, chips)
    far_left = lax.rem(z + half + 1, chips)
    for j in range(RCH):
        cols = pl.ds(j * width, width)
        first = jnp.dot(x2[0, c], w2[c, :, cols], preferred_element_type=F32).astype(BF16).astype(F32)
        second = jnp.dot(x2[1, 0], w2[1 - c, :, cols], preferred_element_type=F32).astype(BF16).astype(F32)
        p[:, cols] = first + second
        rs[0, 0, j] = block_of(far, cols).astype(BF16)
        ring(0, 0, j).start()
        rs[1, 0, j] = block_of(far_left, cols).astype(BF16)
        ring(1, 0, j).start()

    def hop(s, carry):
        cw = lax.rem(z + half - s, chips)
        ccw = lax.rem(z + half + 1 + s, chips)
        for j in range(RCH):
            cols = pl.ds(j * width, width)
            ring(0, s - 1, j).wait_recv()
            rs[0, s, j] = (block_of(cw, cols) + rr[0, s - 1, j].astype(F32)).astype(BF16)
            ring(0, s, j).start()

            @pl.when(s < half - 1)
            def _():
                ring(1, s - 1, j).wait_recv()
                rs[1, s, j] = (block_of(ccw, cols) + rr[1, s - 1, j].astype(F32)).astype(BF16)
                ring(1, s, j).start()

        return carry

    lax.fori_loop(1, half, hop, 0)
    for j in range(RCH):
        cols = pl.ds(j * width, width)
        ring(0, half - 1, j).wait_recv()
        ring(1, half - 2, j).wait_recv()
        total = block_of(z, cols) + rr[0, half - 1, j].astype(F32) + rr[1, half - 2, j].astype(F32)
        out[:, cols] = (hidden[:, cols].astype(F32) + total).astype(BF16)

    def drain(s, carry):
        for j in range(RCH):
            ring(0, s, j).wait_send()

            @pl.when(s < half - 1)
            def _():
                ring(1, s, j).wait_send()

        return carry

    lax.fori_loop(0, half, drain, 0)


def local(
    hidden_in,
    norm_gain,
    w_query,
    w_kv,
    w_out,
    prefix_keys,
    prefix_values,
    suffix_keys,
    suffix_values,
    row_counts,
    suffix_lengths,
):
    chips = lax.axis_size("tensor_0")
    devices = 2 * chips
    my_index = lax.axis_index(TENSOR)
    own, width = hidden_in.shape
    heads = w_kv.shape[1]
    pair = w_query.shape[1]
    groups = devices // heads
    prompts = row_counts.shape[0]
    per_group = prompts // groups
    rows = suffix_lengths.shape[0]
    slab = w_kv.shape[0]
    half = chips // 2
    vmem = pl.BlockSpec(memory_space=pltpu.VMEM)
    anywhere = pl.BlockSpec(memory_space=pl.ANY)
    dma = pltpu.SemaphoreType.DMA

    slot = jnp.arange(groups * PAD, dtype=jnp.int32)
    inside = slot % PAD
    prompt = slot // PAD * per_group + inside // PCAP
    offset = inside % PCAP
    ids = jnp.arange(prompts, dtype=jnp.int32)[None, :]
    start = jnp.sum(jnp.where(ids < prompt[:, None], row_counts[None, :], 0), axis=1)
    count = jnp.sum(jnp.where(ids == prompt[:, None], row_counts[None, :], 0), axis=1)
    used = (inside < per_group * PCAP) & (offset < count)
    slot_row = jnp.where(used, start + offset, -1).astype(jnp.int32)
    mine = lax.dynamic_slice_in_dim(slot_row, my_index // heads * PAD, PAD, 0)
    hit = mine[:, None] == jnp.arange(rows, dtype=jnp.int32)[None, :]
    lens = jnp.maximum(jnp.sum(jnp.where(hit, suffix_lengths[None, :], 0), axis=1), 1).astype(jnp.int32)

    frequency = 500000.0 ** (-(2.0 * jnp.arange(HD // 2, dtype=F32)) / HD)
    angle = (PREFIX + suffix_lengths).astype(F32)[:, None] * frequency[None, :]
    cosines, sines = jnp.cos(angle), jnp.sin(angle)
    cosf = jnp.concatenate([cosines, cosines], axis=1)
    sinf = jnp.concatenate([-sines, sines], axis=1)

    q_slots, kv_slots = pl.pallas_call(
        functools.partial(project_kernel, chips),
        out_shape=(
            jax.ShapeDtypeStruct((groups, PAD, pair * HD), BF16),
            jax.ShapeDtypeStruct((PAD, 2 * HD), BF16),
        ),
        in_specs=[vmem, vmem, anywhere, anywhere, vmem, vmem, vmem],
        out_specs=(vmem, vmem),
        scratch_shapes=[
            pltpu.VMEM((devices, own, width), BF16),
            pltpu.VMEM((width, pair * HD), BF16),
            pltpu.VMEM((2 * slab, heads * 2 * HD), BF16),
            pltpu.VMEM((2, half, own, heads * 2 * HD), KVT),
            pltpu.VMEM((2, half, own, heads * 2 * HD), KVT),
            pltpu.VMEM((groups, PAD, pair * HD), BF16),
            pltpu.VMEM((heads, own, 2 * HD), BF16),
            pltpu.VMEM((devices, own, 2 * HD), BF16),
            dma, dma, dma, dma,
            dma((2, half, XCH)), dma((2, half, XCH)),
            dma((2, half + 1)), dma((2, half + 1)),
            dma((2, half)), dma((2, half)),
            dma((groups,)), dma((groups,)), dma,
            dma((devices,)), dma((devices,)), dma,
        ],
        compiler_params=pltpu.CompilerParams(collective_id=0, has_side_effects=True),
    )(
        hidden_in,
        norm_gain.reshape(1, width),
        w_query.reshape(width, pair * HD),
        w_kv.reshape(slab, heads * 2 * HD),
        cosf,
        sinf,
        slot_row.reshape(groups * PAD, 1),
    )

    keys, size = prefix_keys.shape[2], suffix_keys.shape[2]
    per = groups * pair
    attended = pl.pallas_call(
        attend_kernel,
        grid_spec=pltpu.PrefetchScalarGridSpec(
            num_scalar_prefetch=1,
            grid=(per_group,),
            in_specs=[
                pl.BlockSpec((groups, PAD, pair * HD), lambda i, s: (0, 0, 0)),
                pl.BlockSpec((PAD, 2 * HD), lambda i, s: (0, 0)),
                pl.BlockSpec((1, keys, HD), lambda i, s: (i, 0, 0)),
                pl.BlockSpec((1, keys, HD), lambda i, s: (i, 0, 0)),
                pl.BlockSpec((PCAP, size, HD), lambda i, s: (i, 0, 0)),
                pl.BlockSpec((PCAP, size, HD), lambda i, s: (i, 0, 0)),
            ],
            out_specs=pl.BlockSpec((groups, PAD, pair * HD), lambda i, s: (0, 0, 0)),
            scratch_shapes=[
                pltpu.VMEM((PAD * per, HD), F32),
                pltpu.VMEM((PAD * per, HD), F32),
                pltpu.VMEM((PAD * per, HD), F32),
                pltpu.VMEM((PCAP * per, size), F32),
                pltpu.VMEM((PCAP * per, HD), F32),
                pltpu.VMEM((PAD * per, HD), F32),
            ],
        ),
        out_shape=jax.ShapeDtypeStruct((groups, PAD, pair * HD), BF16),
        compiler_params=pltpu.CompilerParams(dimension_semantics=("arbitrary",)),
    )(lens, q_slots, kv_slots, prefix_keys[0], prefix_values[0], suffix_keys[0], suffix_values[0])

    return pl.pallas_call(
        functools.partial(output_kernel, chips),
        out_shape=jax.ShapeDtypeStruct((own, width), BF16),
        in_specs=[vmem, vmem, anywhere, vmem],
        out_specs=vmem,
        scratch_shapes=[
            pltpu.VMEM((groups, PAD, pair * HD), BF16),
            pltpu.VMEM((2, pair * HD, width), BF16),
            pltpu.VMEM((2, 2, rows // 2, pair * HD), BF16),
            pltpu.VMEM((rows // 2, width), F32),
            pltpu.VMEM((2, half, RCH, own, width // RCH), BF16),
            pltpu.VMEM((2, half, RCH, own, width // RCH), BF16),
            dma, dma, dma,
            dma((groups,)), dma((groups,)), dma,
            dma, dma,
            dma((2, half, RCH)), dma((2, half, RCH)),
        ],
        compiler_params=pltpu.CompilerParams(collective_id=1, has_side_effects=True),
    )(hidden_in, attended, w_out.reshape(pair * HD, width), slot_row.reshape(1, groups * PAD))


def solution(mesh):
    cores = 2
    split = Mesh(
        mesh.devices.reshape(mesh.shape["groups"], mesh.shape["tensor"] // cores, cores),
        ("groups", "tensor_0", "tensor_1"),
    )
    return jax.shard_map(
        local,
        mesh=split,
        in_specs=(
            P(GROUPS_TENSOR, None),
            P(),
            P(None, TENSOR, None),
            P(TENSOR, None, None, None),
            P(TENSOR, None, None),
            P(GROUPS_TENSOR, None, None, None),
            P(GROUPS_TENSOR, None, None, None),
            P(GROUPS_TENSOR, None, None, None),
            P(GROUPS_TENSOR, None, None, None),
            P("groups"),
            P("groups"),
        ),
        out_specs=P(GROUPS_TENSOR, None),
        check_vma=False,
    )
```

```python
import functools
import math

import jax
import jax.numpy as jnp
from jax import lax
from jax.experimental import pallas as pl
from jax.experimental.pallas import tpu as pltpu
from jax.sharding import Mesh
from jax.sharding import PartitionSpec as P

HD = 128
PREFIX = 2048
PCAP = 21
PAIR = 2
CHUNK = 48
TENSOR = ("tensor_0", "tensor_1")
GROUPS_TENSOR = ("groups", "tensor_0", "tensor_1")
MESH = pl.DeviceIdType.MESH
KVT = jnp.bfloat16
XCH = 4
RCH = 8
F32 = jnp.float32
BF16 = jnp.bfloat16
PIECE = 512


def at(z, c):
    return {"tensor_0": z, "tensor_1": c}


def remote(src, dst, send, recv, z, c):
    return pltpu.make_async_remote_copy(
        src_ref=src, dst_ref=dst, send_sem=send, recv_sem=recv, device_id=at(z, c), device_id_type=MESH
    )


def layer_kernel(
    chips, hidden, gain, wq_hbm, wkv_hbm, wo_hbm, pk_hbm, pv_hbm, sk_hbm, sv_hbm, cosf, sinf, counts, lengths, out,
    x, wq_raw, wq, wkv_raw, wkv, wide_f, kvs, kvr, qs, ql, kvh, kvl, table, starts,
    pk, pv, sk, sv, qf, kf, vf, ss, pvacc, attf, ao, a, w2, x2, p, rs, rr,
    wq_sem, wkv_sem, wkvs_sem, wkvr_sem, wo_sem, wos, wor, cache_sem,
    xs, xr, ps, pr, ks, kr, qss, qrs, qls, as_, ar, al, ass, ars, als, xss, xrs, rss, rsr,
):
    z = lax.axis_index("tensor_0")
    c = lax.axis_index("tensor_1")
    devices = 2 * chips
    half = chips // 2
    me = 2 * z + c
    right = lax.rem(z + 1, chips)
    left = lax.rem(z + chips - 1, chips)
    slab = wkv.shape[0] // 2
    features = x.shape[2]
    width = features // XCH
    rows = devices * 8
    groups, chunks = qs.shape[0], qs.shape[1]
    heads = kvh.shape[0]
    per_group = pk.shape[0]
    per = heads
    my_group = me // heads
    my_head = lax.rem(me, heads)
    scaling = 1.0 / math.sqrt(HD)
    barrier = pltpu.get_barrier_semaphore()
    for peer in ((right, c), (left, c), (z, 1 - c)):
        pl.semaphore_signal(barrier, inc=1, device_id=at(*peer), device_id_type=MESH)

    load_wkv = pltpu.make_async_copy(wkv_hbm, wkv_raw, wkv_sem)
    load_wkv.start()
    load_wq = pltpu.make_async_copy(wq_hbm, wq_raw, wq_sem)
    load_wq.start()

    wide = hidden[...].astype(F32)
    inverse = lax.rsqrt(jnp.mean(wide * wide, axis=1, keepdims=True) + 1e-05)
    for j in range(features // HD):
        cols = slice(j * HD, (j + 1) * HD)
        part = hidden[:, cols].astype(F32) * inverse * gain[j : j + 1, :].astype(F32)
        x[me, :, cols] = part.astype(BF16)
    kvs[1, 0] = jnp.zeros(kvs.shape[2:], kvs.dtype)
    own_rows = pl.ds(pl.multiple_of(c * slab, slab), slab)
    load_wkv.wait()
    columns = wkv.shape[1] // HD
    step_rows = PIECE // columns
    for n in range(slab // step_rows):
        wide_f[...] = wkv_raw[n * PIECE : (n + 1) * PIECE, :].astype(F32)
        target = pl.ds(pl.multiple_of(c * slab + n * step_rows, step_rows), step_rows)
        for i in range(columns):
            wkv[target, i * HD : (i + 1) * HD] = wide_f[pl.ds(i, step_rows, stride=columns), :].astype(BF16)

    pl.semaphore_wait(barrier, 3)

    def row_copy(way, step, j, shard):
        piece = x.at[shard, :, pl.ds(j * width, width)]
        return remote(piece, piece, xs.at[way, step, j], xr.at[way, step, j], right if way == 0 else left, c)

    def part_copy(way, step, shard):
        return remote(x.at[shard], x.at[shard], ps.at[way, step], pr.at[way, step], z, 1 - c)

    def kv_copy(way, step):
        return remote(kvs.at[way, step], kvr.at[way, step], ks.at[way, step], kr.at[way, step], right if way == 0 else left, c)

    for j in range(XCH):
        row_copy(0, 0, j, me).start()
        row_copy(1, 0, j, me).start()
    send_wkv = remote(wkv.at[own_rows, :], wkv.at[own_rows, :], wkvs_sem, wkvr_sem, z, 1 - c)
    send_wkv.start()
    part_copy(0, 0, me).start()
    kv_copy(1, 0).start()
    feats = pl.ds(pl.multiple_of(z * 2 * slab, 2 * slab), 2 * slab)

    loads = [
        pltpu.make_async_copy(pk_hbm, pk, cache_sem.at[0]),
        pltpu.make_async_copy(pv_hbm, pv, cache_sem.at[1]),
        pltpu.make_async_copy(sk_hbm, sk, cache_sem.at[2]),
        pltpu.make_async_copy(sv_hbm, sv, cache_sem.at[3]),
        pltpu.make_async_copy(wo_hbm, w2.at[c], wo_sem),
    ]

    running = jnp.int32(0)
    for n in range(groups * per_group):
        starts[n] = running
        running = running + counts[n]

    def slot_ids(g, k, shape, dim):
        index = lax.broadcasted_iota(jnp.int32, shape, dim)
        ids = jnp.full(shape, -1, jnp.int32)
        for u in range(PAIR):
            prompt = g * per_group + k * PAIR + u
            offset = index - u * PCAP
            ids = jnp.where((offset >= 0) & (offset < counts[prompt]), offset + starts[prompt], ids)
        return ids

    send_wkv.wait()
    own = jnp.dot(x[me, :, feats], wkv[...], preferred_element_type=F32)
    kvs[0, 0] = own.astype(kvs.dtype)
    kv_copy(0, 0).start()
    load_wq.wait()
    for load in loads:
        load.start()

    def relay(n):
        wide_f[...] = wq_raw[pl.ds(pl.multiple_of(n * PIECE, PIECE), PIECE), :].astype(F32)
        target = pl.ds(pl.multiple_of(n * (PIECE // 2), PIECE // 2), PIECE // 2)
        for i in range(2):
            wq[target, i * HD : (i + 1) * HD] = wide_f[pl.ds(i, PIECE // 2, stride=2), :].astype(BF16)

    pieces = 2 * features // PIECE // half
    for n in range(pieces):
        relay(n)

    def hop(s, carry):
        cw = 2 * lax.rem(z - s + chips, chips) + c
        ccw = 2 * lax.rem(z + s, chips) + c
        for j in range(XCH):
            row_copy(0, s - 1, j, cw).wait_recv()
            row_copy(0, s, j, cw).start()
            row_copy(1, s - 1, j, ccw).wait_recv()

            @pl.when(s < half - 1)
            def _():
                row_copy(1, s, j, ccw).start()

        part_copy(0, s, cw).start()
        part_copy(1, s, ccw).start()
        both = jnp.concatenate([x[cw, :, feats].astype(F32), x[ccw, :, feats].astype(F32)], axis=0).astype(BF16)
        part = jnp.dot(both, wkv[...], preferred_element_type=F32)
        kv_copy(0, s - 1).wait_recv()
        kvs[0, s] = (part[:8] + kvr[0, s - 1].astype(F32)).astype(kvs.dtype)
        kv_copy(0, s).start()
        kv_copy(1, s - 1).wait_recv()
        kvs[1, s] = (part[8:] + kvr[1, s - 1].astype(F32)).astype(kvs.dtype)
        kv_copy(1, s).start()
        for n in range(pieces):
            relay(s * pieces + n)
        return carry

    lax.fori_loop(1, half, hop, 0)
    far = 2 * lax.rem(z + half, chips) + c
    for j in range(XCH):
        row_copy(0, half - 1, j, far).wait_recv()
    part_copy(0, half, far).start()
    own = jnp.dot(x[far, :, feats], wkv[...], preferred_element_type=F32)
    kv_copy(0, half - 1).wait_recv()
    kv_copy(1, half - 1).wait_recv()
    kv_raw = (own + kvr[0, half - 1].astype(F32) + kvr[1, half - 1].astype(F32)).astype(BF16).astype(F32)
    far_rows = pl.ds(pl.multiple_of(far * 8, 8), 8)
    cos8 = cosf[far_rows, :]
    sin8 = sinf[far_rows, :]
    for h in range(heads):
        key = kv_raw[:, h * 2 * HD : h * 2 * HD + HD]
        value = kv_raw[:, h * 2 * HD + HD : (h + 1) * 2 * HD]
        kvh[h, :, :HD] = (key * cos8 + pltpu.roll(key, HD // 2, 1) * sin8).astype(BF16)
        kvh[h, :, HD:] = value.astype(BF16)

    def kv_send(n):
        return remote(kvh.at[lax.rem(n, heads)], kvl.at[far], as_.at[n], ar.at[far], n // 2, lax.rem(n, 2))

    kv_self = pltpu.make_async_copy(kvh.at[my_head], kvl.at[far], al)

    part_copy(0, 0, me).wait_recv()

    def part_wait(s, carry):
        part_copy(0, s, me).wait_recv()
        part_copy(1, s, me).wait_recv()
        return carry

    lax.fori_loop(1, half, part_wait, 0)
    part_copy(0, half, me).wait_recv()

    def kv_out_loop(n, carry):
        @pl.when(n != me)
        def _():
            kv_send(n).start()

        return carry

    lax.fori_loop(0, devices, kv_out_loop, 0)
    kv_self.start()
    depth = 1024

    def q_step(k, acc):
        piece = pl.ds(pl.multiple_of(k * depth, depth), depth)
        xk = x[:, :, piece].astype(F32).reshape(rows, depth).astype(BF16)
        return acc + jnp.dot(xk, wq[piece, :], preferred_element_type=F32)

    acc = lax.fori_loop(0, features // depth, q_step, jnp.zeros((rows, 2 * HD), F32))
    q_raw = acc.astype(BF16).astype(F32)
    roped = []
    for j in range(2):
        v = q_raw[:, j * HD : (j + 1) * HD]
        roped.append((v * cosf[...] + pltpu.roll(v, HD // 2, 1) * sinf[...]).astype(BF16))
    roped = jnp.concatenate(roped, axis=1)
    block = 2 * lax.rem(z, 2) + c

    def select(ids, dim):
        return jnp.where(lax.broadcasted_iota(jnp.int32, ids.shape, dim) == ids, 1.0, 0.0).astype(BF16)

    def q_send(g, k):
        owner = heads * g + z // 2
        return remote(qs.at[g, k], ql.at[block, k], qss.at[g, k], qrs.at[block, k], owner // 2, lax.rem(owner, 2))

    def q_local(g, k):
        return pltpu.make_async_copy(qs.at[g, k], ql.at[block, k], qls.at[k])

    for k in range(chunks):
        for g in range(groups):
            pick = select(slot_ids(g, k, (CHUNK, rows), 0), 1)
            qs[g, k] = jnp.dot(pick, roped, preferred_element_type=F32).astype(BF16)
            owner = heads * g + z // 2

            @pl.when(owner != me)
            def _():
                q_send(g, k).start()

            @pl.when(owner == me)
            def _():
                q_local(g, k).start()

    send_w = remote(wo_hbm, w2.at[c], wos, wor, z, 1 - c)
    send_w.start()
    attf[...] = jnp.zeros_like(attf)

    def kv_in_loop(n, carry):
        @pl.when(n != far)
        def _():
            remote(kvh.at[0], kvl.at[n], as_.at[0], ar.at[n], z, 1 - c).wait_recv()

        return carry

    lax.fori_loop(0, devices, kv_in_loop, 0)
    kv_self.wait()
    table[...] = kvl[...].astype(F32).reshape(rows, 2 * HD).astype(BF16)
    for load in loads:
        load.wait()

    def a_send(b, k):
        dest = groups * my_head + b
        return remote(ao.at[b, k], a.at[my_group, k], ass.at[b, k], ars.at[my_group, k], dest // 2, lax.rem(dest, 2))

    def a_local(b, k):
        return pltpu.make_async_copy(ao.at[b, k], a.at[my_group, k], als.at[k])

    span = PCAP * per
    contract = (((1,), (1,)), ((), ()))

    def attend(i, carry):
        k, u = i // PAIR, lax.rem(i, PAIR)

        @pl.when(u == 0)
        def _():
            pick = select(slot_ids(my_group, k, (CHUNK, rows), 0), 1)
            kv = jnp.dot(pick, table[...], preferred_element_type=F32)
            for j in range(per):
                kf[pl.ds(j, CHUNK, stride=per), :] = kv[:, :HD]
                vf[pl.ds(j, CHUNK, stride=per), :] = kv[:, HD:]
            for b in range(groups):
                source = groups * my_head + b

                @pl.when(source != me)
                def _():
                    remote(qs.at[0, 0], ql.at[b, k], qss.at[0, 0], qrs.at[b, k], z, 1 - c).wait_recv()

                @pl.when(source == me)
                def _():
                    q_local(0, k).wait()

            for j in range(per):
                qf[pl.ds(j, CHUNK, stride=per), :] = ql[j // 2, k, :, (j % 2) * HD : (j % 2 + 1) * HD].astype(F32)

        mine = pl.ds(pl.multiple_of(u * span, 8), span)
        qi = qf[mine, :]
        prompt = my_group * per_group + i
        first_row = starts[prompt]
        pscore = lax.dot_general(qi.astype(BF16), pk[i], contract, preferred_element_type=F32) * scaling
        for r in range(PCAP):
            q8 = qf[pl.ds(pl.multiple_of(u * span + r * per, 8), per), :].astype(BF16)
            s8 = lax.dot_general(q8, sk[i * PCAP + r], contract, preferred_element_type=F32) * scaling
            length = lengths[jnp.minimum(first_row + r, rows - 1)]
            seen = lax.broadcasted_iota(jnp.int32, s8.shape, 1) < length
            ss[r * per : (r + 1) * per, :] = jnp.where(seen, s8, -jnp.inf)
        self_score = jnp.sum(qi * kf[mine, :], axis=1, keepdims=True) * scaling
        sfx = ss[...]
        top = jnp.maximum(
            jnp.max(pscore, axis=1, keepdims=True), jnp.maximum(jnp.max(sfx, axis=1, keepdims=True), self_score)
        )
        pe = jnp.exp(pscore - top)
        se = jnp.exp(sfx - top)
        own = jnp.exp(self_score - top)
        total = jnp.sum(pe, axis=1, keepdims=True) + jnp.sum(se, axis=1, keepdims=True) + own
        acc = jnp.dot(pe.astype(BF16), pv[i], preferred_element_type=F32)
        ss[...] = se
        for r in range(PCAP):
            w8 = ss[r * per : (r + 1) * per, :].astype(BF16)
            pvacc[r * per : (r + 1) * per, :] = jnp.dot(w8, sv[i * PCAP + r], preferred_element_type=F32)
        attf[mine, :] = (acc + pvacc[...] + own * vf[mine, :]) / total

        @pl.when(u == PAIR - 1)
        def _():
            for j in range(per):
                ao[j // 2, k, :, (j % 2) * HD : (j % 2 + 1) * HD] = attf[pl.ds(j, CHUNK, stride=per), :].astype(BF16)
            for b in range(groups):
                dest = groups * my_head + b

                @pl.when(dest != me)
                def _():
                    a_send(b, k).start()

                @pl.when(dest == me)
                def _():
                    a_local(b, k).start()

        return carry

    lax.fori_loop(0, per_group, attend, 0)

    order = lax.broadcasted_iota(jnp.int32, (rows, CHUNK), 0)
    wanted = (lax.rem(order, rows // 2) // 8 * 2 + order // (rows // 2)) * 8 + lax.rem(order, 8)
    picked = jnp.zeros((rows, 2 * HD), F32)
    for k in range(chunks):
        for g in range(groups):
            source = heads * g + me // groups

            @pl.when(source != me)
            def _():
                remote(ao.at[0, 0], a.at[g, k], ass.at[0, 0], ars.at[g, k], z, 1 - c).wait_recv()

            @pl.when(source == me)
            def _():
                a_local(0, k).wait()

            pick = jnp.where(wanted == slot_ids(g, k, (rows, CHUNK), 1), 1.0, 0.0).astype(BF16)
            picked = picked + jnp.dot(pick, a[g, k], preferred_element_type=F32)
    x2[0, 0] = picked[: rows // 2].astype(BF16)
    x2[0, 1] = picked[rows // 2 :].astype(BF16)
    swap = remote(x2.at[0, 1 - c], x2.at[1, 0], xss, xrs, z, 1 - c)
    swap.start()
    send_w.wait()
    rwidth = features // RCH
    ready = 3

    def own_part(j):
        cols = pl.ds(j * rwidth, rwidth)
        p[:, cols] = jnp.dot(x2[0, c], w2[c, :, cols], preferred_element_type=F32).astype(BF16).astype(F32)

    for j in range(ready):
        own_part(j)
    swap.wait()

    def ring(way, step, j):
        return remote(
            rs.at[way, step, j], rr.at[way, step, j], rss.at[way, step, j], rsr.at[way, step, j],
            right if way == 0 else left, c,
        )

    def block_of(chip, cols):
        return p[pl.ds(pl.multiple_of(chip * 8, 8), 8), cols]

    far_chip = lax.rem(z + half, chips)
    far_left = lax.rem(z + half + 1, chips)
    for j in range(RCH):
        if j >= ready:
            own_part(j)
        cols = pl.ds(j * rwidth, rwidth)
        second = jnp.dot(x2[1, 0], w2[1 - c, :, cols], preferred_element_type=F32).astype(BF16).astype(F32)
        p[:, cols] = p[:, cols] + second
        rs[0, 0, j] = block_of(far_chip, cols).astype(BF16)
        ring(0, 0, j).start()
        rs[1, 0, j] = block_of(far_left, cols).astype(BF16)
        ring(1, 0, j).start()

    def fold(s, carry):
        cw = lax.rem(z + half - s, chips)
        ccw = lax.rem(z + half + 1 + s, chips)
        for j in range(RCH):
            cols = pl.ds(j * rwidth, rwidth)
            ring(0, s - 1, j).wait_recv()
            rs[0, s, j] = (block_of(cw, cols) + rr[0, s - 1, j].astype(F32)).astype(BF16)
            ring(0, s, j).start()

            @pl.when(s < half - 1)
            def _():
                ring(1, s - 1, j).wait_recv()
                rs[1, s, j] = (block_of(ccw, cols) + rr[1, s - 1, j].astype(F32)).astype(BF16)
                ring(1, s, j).start()

        return carry

    lax.fori_loop(1, half, fold, 0)
    for j in range(RCH):
        cols = pl.ds(j * rwidth, rwidth)
        ring(0, half - 1, j).wait_recv()
        ring(1, half - 2, j).wait_recv()
        total = block_of(z, cols) + rr[0, half - 1, j].astype(F32) + rr[1, half - 2, j].astype(F32)
        out[:, cols] = (hidden[:, cols].astype(F32) + total).astype(BF16)

    for j in range(XCH):
        row_copy(0, 0, j, me).wait_send()
        row_copy(1, 0, j, me).wait_send()
    part_copy(0, 0, me).wait_send()
    part_copy(0, half, me).wait_send()
    kv_copy(0, 0).wait_send()
    kv_copy(1, 0).wait_send()
    for j in range(RCH):
        ring(0, 0, j).wait_send()
        ring(1, 0, j).wait_send()

    def drain(s, carry):
        for j in range(XCH):
            row_copy(0, s, j, me).wait_send()

            @pl.when(s < half - 1)
            def _():
                row_copy(1, s, j, me).wait_send()

        part_copy(0, s, me).wait_send()
        part_copy(1, s, me).wait_send()
        kv_copy(0, s).wait_send()
        kv_copy(1, s).wait_send()
        for j in range(RCH):
            ring(0, s, j).wait_send()

            @pl.when(s < half - 1)
            def _():
                ring(1, s, j).wait_send()

        return carry

    lax.fori_loop(1, half, drain, 0)

    def kv_drain(n, carry):
        @pl.when(n != me)
        def _():
            kv_send(n).wait_send()

        return carry

    lax.fori_loop(0, devices, kv_drain, 0)
    for k in range(chunks):
        for g in range(groups):
            owner = heads * g + z // 2
            dest = groups * my_head + g

            @pl.when(owner != me)
            def _():
                q_send(g, k).wait_send()

            @pl.when(dest != me)
            def _():
                a_send(g, k).wait_send()


def local(
    hidden_in,
    norm_gain,
    w_query,
    w_kv,
    w_out,
    prefix_keys,
    prefix_values,
    suffix_keys,
    suffix_values,
    row_counts,
    suffix_lengths,
):
    chips = lax.axis_size("tensor_0")
    devices = 2 * chips
    own, width = hidden_in.shape
    heads = w_kv.shape[1]
    pair = w_query.shape[1]
    groups = devices // heads
    per_group = row_counts.shape[0] // groups
    chunks = per_group // PAIR
    rows = suffix_lengths.shape[0]
    slab = w_kv.shape[0]
    half = chips // 2
    keys, size = prefix_keys.shape[2], suffix_keys.shape[2]
    columns = heads * 2 * HD
    vmem = pl.BlockSpec(memory_space=pltpu.VMEM)
    smem = pl.BlockSpec(memory_space=pltpu.SMEM)
    anywhere = pl.BlockSpec(memory_space=pl.ANY)
    dma = pltpu.SemaphoreType.DMA

    frequency = 500000.0 ** (-(2.0 * (jnp.arange(HD) % (HD // 2)).astype(F32)) / HD)
    angle = (PREFIX + suffix_lengths).astype(F32)[:, None] * frequency[None, :]
    cosf = jnp.cos(angle)
    sinf = jnp.where(jnp.arange(HD) < HD // 2, -1.0, 1.0)[None, :] * jnp.sin(angle)

    slots = (groups, chunks, CHUNK, pair * HD)
    return pl.pallas_call(
        functools.partial(layer_kernel, chips),
        out_shape=jax.ShapeDtypeStruct((own, width), BF16),
        in_specs=[vmem, vmem] + [anywhere] * 7 + [vmem, vmem, smem, smem],
        out_specs=vmem,
        scratch_shapes=[
            pltpu.VMEM((devices, own, width), BF16),
            pltpu.VMEM((width * pair, HD), BF16),
            pltpu.VMEM((width, pair * HD), BF16),
            pltpu.VMEM((slab * heads * 2, HD), BF16),
            pltpu.VMEM((2 * slab, columns), BF16),
            pltpu.VMEM((PIECE, HD), F32),
            pltpu.VMEM((2, half, own, columns), KVT),
            pltpu.VMEM((2, half, own, columns), KVT),
            pltpu.VMEM(slots, BF16),
            pltpu.VMEM(slots, BF16),
            pltpu.VMEM((heads, own, 2 * HD), BF16),
            pltpu.VMEM((devices, own, 2 * HD), BF16),
            pltpu.VMEM((rows, 2 * HD), BF16),
            pltpu.SMEM((groups * per_group,), jnp.int32),
            pltpu.VMEM((per_group, keys, HD), BF16),
            pltpu.VMEM((per_group, keys, HD), BF16),
            pltpu.VMEM((per_group * PCAP, size, HD), BF16),
            pltpu.VMEM((per_group * PCAP, size, HD), BF16),
            pltpu.VMEM((CHUNK * heads, HD), F32),
            pltpu.VMEM((CHUNK * heads, HD), F32),
            pltpu.VMEM((CHUNK * heads, HD), F32),
            pltpu.VMEM((PCAP * heads, size), F32),
            pltpu.VMEM((PCAP * heads, HD), F32),
            pltpu.VMEM((CHUNK * heads, HD), F32),
            pltpu.VMEM(slots, BF16),
            pltpu.VMEM(slots, BF16),
            pltpu.VMEM((2, pair * HD, width), BF16),
            pltpu.VMEM((2, 2, rows // 2, pair * HD), BF16),
            pltpu.VMEM((rows // 2, width), F32),
            pltpu.VMEM((2, half, RCH, own, width // RCH), BF16),
            pltpu.VMEM((2, half, RCH, own, width // RCH), BF16),
            dma, dma, dma, dma, dma, dma, dma, dma((4,)),
            dma((2, half, XCH)), dma((2, half, XCH)),
            dma((2, half + 1)), dma((2, half + 1)),
            dma((2, half)), dma((2, half)),
            dma((groups, chunks)), dma((groups, chunks)), dma((chunks,)),
            dma((devices,)), dma((devices,)), dma,
            dma((groups, chunks)), dma((groups, chunks)), dma((chunks,)),
            dma, dma,
            dma((2, half, RCH)), dma((2, half, RCH)),
        ],
        compiler_params=pltpu.CompilerParams(
            collective_id=0, has_side_effects=True, vmem_limit_bytes=66_000_000
        ),
    )(
        hidden_in,
        norm_gain.reshape(width // HD, HD),
        w_query.reshape(width * pair, HD),
        w_kv.reshape(slab * heads * 2, HD),
        w_out.reshape(pair * HD, width),
        prefix_keys[0],
        prefix_values[0],
        suffix_keys[0],
        suffix_values[0],
        cosf,
        sinf,
        row_counts,
        suffix_lengths,
    )


def solution(mesh):
    cores = 2
    split = Mesh(
        mesh.devices.reshape(mesh.shape["groups"], mesh.shape["tensor"] // cores, cores),
        ("groups", "tensor_0", "tensor_1"),
    )
    return jax.shard_map(
        local,
        mesh=split,
        in_specs=(
            P(GROUPS_TENSOR, None),
            P(),
            P(None, TENSOR, None),
            P(TENSOR, None, None, None),
            P(TENSOR, None, None),
            P(GROUPS_TENSOR, None, None, None),
            P(GROUPS_TENSOR, None, None, None),
            P(GROUPS_TENSOR, None, None, None),
            P(GROUPS_TENSOR, None, None, None),
            P("groups"),
            P("groups"),
        ),
        out_specs=P(GROUPS_TENSOR, None),
        check_vma=False,
    )
```

```python
import functools
import math

import jax
import jax.numpy as jnp
from jax import lax
from jax.experimental import pallas as pl
from jax.experimental.pallas import tpu as pltpu
from jax.sharding import Mesh
from jax.sharding import PartitionSpec as P

HD = 128
PREFIX = 2048
PCAP = 21
PAIR = 3
CHUNK = 64
TENSOR = ("tensor_0", "tensor_1")
GROUPS_TENSOR = ("groups", "tensor_0", "tensor_1")
MESH = pl.DeviceIdType.MESH
KVT = jnp.bfloat16
XCH = 4
RCH = 8
F32 = jnp.float32
BF16 = jnp.bfloat16
PIECE = 512


def at(z, c):
    return {"tensor_0": z, "tensor_1": c}


def remote(src, dst, send, recv, z, c):
    return pltpu.make_async_remote_copy(
        src_ref=src, dst_ref=dst, send_sem=send, recv_sem=recv, device_id=at(z, c), device_id_type=MESH
    )


def layer_kernel(
    chips, hidden, gain, wq_hbm, wkv_hbm, wo_hbm, pk_hbm, pv_hbm, sk_hbm, sv_hbm, cosf, sinf, counts, lengths, out,
    x, wq_raw, wq, wkv_raw, wkv, wide_f, kvs, kvr, qs, ql, kvh, kvl, table, starts,
    pk, pv, sk, sv, qf, kf, vf, mf, lf, qt, qacc, ss, pvacc, attf, ao, a, w2, x2, p, rs, rr,
    wq_sem, wkv_sem, wkvs_sem, wkvr_sem, wo_sem, wos, wor, cache_sem,
    xs, xr, ps, pr, ks, kr, qss, qrs, qls, as_, ar, al, ass, ars, als, xss, xrs, rss, rsr,
):
    z = lax.axis_index("tensor_0")
    c = lax.axis_index("tensor_1")
    devices = 2 * chips
    half = chips // 2
    me = 2 * z + c
    right = lax.rem(z + 1, chips)
    left = lax.rem(z + chips - 1, chips)
    slab = wkv.shape[0] // 2
    features = x.shape[2]
    width = features // XCH
    rows = devices * 8
    groups, chunks = qs.shape[0], qs.shape[1]
    heads = kvh.shape[0]
    per_group = pk.shape[0]
    per = heads
    my_group = me // heads
    my_head = lax.rem(me, heads)
    scaling = 1.0 / math.sqrt(HD)
    barrier = pltpu.get_barrier_semaphore()
    for peer in ((right, c), (left, c), (z, 1 - c)):
        pl.semaphore_signal(barrier, inc=1, device_id=at(*peer), device_id_type=MESH)

    load_wkv = pltpu.make_async_copy(wkv_hbm, wkv_raw, wkv_sem)
    load_wkv.start()
    load_wq = pltpu.make_async_copy(wq_hbm, wq_raw, wq_sem)
    load_wq.start()

    wide = hidden[...].astype(F32)
    inverse = lax.rsqrt(jnp.mean(wide * wide, axis=1, keepdims=True) + 1e-05)
    for j in range(features // HD):
        cols = slice(j * HD, (j + 1) * HD)
        part = hidden[:, cols].astype(F32) * inverse * gain[j : j + 1, :].astype(F32)
        x[me, :, cols] = part.astype(BF16)
    pl.semaphore_wait(barrier, 3)

    def row_copy(way, step, j, shard):
        piece = x.at[shard, :, pl.ds(j * width, width)]
        return remote(piece, piece, xs.at[way, step, j], xr.at[way, step, j], right if way == 0 else left, c)

    def part_copy(way, step, shard):
        return remote(x.at[shard], x.at[shard], ps.at[way, step], pr.at[way, step], z, 1 - c)

    def kv_copy(way, step):
        return remote(kvs.at[way, step], kvr.at[way, step], ks.at[way, step], kr.at[way, step], right if way == 0 else left, c)

    for j in range(XCH):
        row_copy(0, 0, j, me).start()
        row_copy(1, 0, j, me).start()
    part_copy(0, 0, me).start()
    kvs[1, 0] = jnp.zeros(kvs.shape[2:], kvs.dtype)
    own_rows = pl.ds(pl.multiple_of(c * slab, slab), slab)
    load_wkv.wait()
    columns = wkv.shape[1] // HD
    step_rows = PIECE // columns
    for n in range(slab // step_rows):
        wide_f[...] = wkv_raw[n * PIECE : (n + 1) * PIECE, :].astype(F32)
        target = pl.ds(pl.multiple_of(c * slab + n * step_rows, step_rows), step_rows)
        for i in range(columns):
            wkv[target, i * HD : (i + 1) * HD] = wide_f[pl.ds(i, step_rows, stride=columns), :].astype(BF16)

    send_wkv = remote(wkv.at[own_rows, :], wkv.at[own_rows, :], wkvs_sem, wkvr_sem, z, 1 - c)
    send_wkv.start()
    kv_copy(1, 0).start()
    feats = pl.ds(pl.multiple_of(z * 2 * slab, 2 * slab), 2 * slab)

    loads = [
        pltpu.make_async_copy(pk_hbm, pk, cache_sem.at[0]),
        pltpu.make_async_copy(pv_hbm, pv, cache_sem.at[1]),
        pltpu.make_async_copy(sk_hbm, sk, cache_sem.at[2]),
        pltpu.make_async_copy(sv_hbm, sv, cache_sem.at[3]),
        pltpu.make_async_copy(wo_hbm, w2.at[c], wo_sem),
    ]

    running = jnp.int32(0)
    for n in range(groups * per_group):
        starts[n] = running
        running = running + counts[n]

    def slot_ids(g, k, shape, dim):
        index = lax.broadcasted_iota(jnp.int32, shape, dim)
        ids = jnp.full(shape, -1, jnp.int32)
        for u in range(PAIR):
            prompt = g * per_group + k * PAIR + u
            offset = index - u * PCAP
            ids = jnp.where((offset >= 0) & (offset < counts[prompt]), offset + starts[prompt], ids)
        return ids

    send_wkv.wait()
    own = jnp.dot(x[me, :, feats], wkv[...], preferred_element_type=F32)
    kvs[0, 0] = own.astype(kvs.dtype)
    kv_copy(0, 0).start()
    load_wq.wait()
    for load in loads:
        load.start()

    def relay(n):
        wide_f[...] = wq_raw[pl.ds(pl.multiple_of(n * PIECE, PIECE), PIECE), :].astype(F32)
        target = pl.ds(pl.multiple_of(n * (PIECE // 2), PIECE // 2), PIECE // 2)
        for i in range(2):
            wq[target, i * HD : (i + 1) * HD] = wide_f[pl.ds(i, PIECE // 2, stride=2), :].astype(BF16)

    early = half // 2
    pieces = 2 * features // PIECE // early
    each = pieces // XCH
    for n in range(pieces):
        relay(n)

    def part_wait(s):
        part_copy(0, s, me).wait_recv()
        part_copy(1, s, me).wait_recv()

    def kv_step(s):
        cw = 2 * lax.rem(z - s + chips, chips) + c
        ccw = 2 * lax.rem(z + s, chips) + c
        both = jnp.concatenate([x[cw, :, feats].astype(F32), x[ccw, :, feats].astype(F32)], axis=0).astype(BF16)
        part = jnp.dot(both, wkv[...], preferred_element_type=F32)
        for way in range(2):
            kv_copy(way, s - 1).wait_recv()
            kvs[way, s] = (part[8 * way : 8 * way + 8] + kvr[way, s - 1].astype(F32)).astype(kvs.dtype)
            kv_copy(way, s).start()

    def shard_of(index, core):
        return 2 * lax.rem(index + 2 * chips, chips) + core

    def project(shards, j):
        cols = pl.ds(j * width, width)
        stacked = jnp.concatenate([x[n, :, cols].astype(F32) for n in shards], axis=0).astype(BF16)
        part = jnp.dot(stacked, wq[j * width : (j + 1) * width, :], preferred_element_type=F32)
        size = len(shards) * 8
        if j == 0:
            qacc[:size] = part
        else:
            qacc[:size] = qacc[:size] + part
        if j == XCH - 1:
            for n, shard in enumerate(shards):
                qt[pl.ds(pl.multiple_of(shard * 8, 8), 8), :] = qacc[n * 8 : n * 8 + 8]

    def hop(s, carry):
        cw = 2 * lax.rem(z - s + chips, chips) + c
        ccw = 2 * lax.rem(z + s, chips) + c

        @pl.when(s == early)
        def _():
            part_copy(0, 0, me).wait_recv()
            part_wait(1)

        @pl.when(s == early + 1)
        def _():
            part_wait(2)
            part_wait(3)

        @pl.when(s == early + 2)
        def _():
            part_wait(4)
            part_wait(5)

        @pl.when(s == early + 3)
        def _():
            part_wait(6)

        late = jnp.minimum(2 * (s - early), half - 2)
        later = jnp.minimum(late + 1, half - 2)
        for j in range(XCH):
            row_copy(0, s - 1, j, cw).wait_recv()

            @pl.when((s < half - 1) | (j < XCH // 2))
            def _():
                row_copy(0, s, j, cw).start()

            row_copy(1, s - 1, j, ccw).wait_recv()

            @pl.when((s < half - 1) | (j >= XCH // 2))
            def _():
                row_copy(1, s, j, ccw).start()

            if j == XCH - 1:
                part_copy(0, s, cw).start()
                part_copy(1, s, ccw).start()

            @pl.when(s < early)
            def _():
                for n in range(each):
                    relay(s * pieces + j * each + n)

            @pl.when(s >= early)
            def _():
                project([shard_of(z + way * n, core) for n in (late, later) for way in (-1, 1) for core in (0, 1)], j)

            if j == XCH - 1:
                kv_step(s)

        return carry

    lax.fori_loop(1, half, hop, 0)
    far = 2 * lax.rem(z + half, chips) + c
    for j in range(XCH):
        row_copy(0 if j < XCH // 2 else 1, half - 1, j, far).wait_recv()
    part_copy(0, half, far).start()
    block = 2 * lax.rem(z, 2) + c
    part_wait(half - 1)
    last = [shard_of(z + way * (half - 1), core) for way in (-1, 1) for core in (0, 1)] + [far]
    part_copy(0, half, me).wait_recv()
    last.append(2 * lax.rem(z + half, chips) + 1 - c)
    for j in range(XCH):
        project(last, j)
    q_raw = qt[...].astype(BF16).astype(F32)
    roped = []
    for j in range(2):
        v = q_raw[:, j * HD : (j + 1) * HD]
        roped.append((v * cosf[...] + pltpu.roll(v, HD // 2, 1) * sinf[...]).astype(BF16))
    roped = jnp.concatenate(roped, axis=1)

    def select(ids, dim):
        return jnp.where(lax.broadcasted_iota(jnp.int32, ids.shape, dim) == ids, 1.0, 0.0).astype(BF16)

    def q_send(g, k):
        owner = heads * g + z // 2
        return remote(qs.at[g, k], ql.at[block, k], qss.at[g, k], qrs.at[block, k], owner // 2, lax.rem(owner, 2))

    def q_local(g, k):
        return pltpu.make_async_copy(qs.at[g, k], ql.at[block, k], qls.at[k])

    def q_out(k):
        for turn in (2, 1, 3, 0):
            g = lax.rem(z // (chips // groups) + turn, groups)
            pick = select(slot_ids(g, k, (CHUNK, rows), 0), 1)
            qs[g, k] = jnp.dot(pick, roped, preferred_element_type=F32).astype(BF16)
            owner = heads * g + z // 2

            @pl.when(owner != me)
            def _():
                q_send(g, k).start()

            @pl.when(owner == me)
            def _():
                q_local(g, k).start()

    q_out(0)
    own = jnp.dot(x[far, :, feats], wkv[...], preferred_element_type=F32)
    kv_copy(0, half - 1).wait_recv()
    kv_copy(1, half - 1).wait_recv()
    kv_raw = (own + kvr[0, half - 1].astype(F32) + kvr[1, half - 1].astype(F32)).astype(BF16).astype(F32)
    far_rows = pl.ds(pl.multiple_of(far * 8, 8), 8)
    cos8 = cosf[far_rows, :]
    sin8 = sinf[far_rows, :]
    for h in range(heads):
        key = kv_raw[:, h * 2 * HD : h * 2 * HD + HD]
        value = kv_raw[:, h * 2 * HD + HD : (h + 1) * 2 * HD]
        kvh[h, :, :HD] = (key * cos8 + pltpu.roll(key, HD // 2, 1) * sin8).astype(BF16)
        kvh[h, :, HD:] = value.astype(BF16)

    def kv_send(n):
        return remote(kvh.at[lax.rem(n, heads)], kvl.at[far], as_.at[n], ar.at[far], n // 2, lax.rem(n, 2))

    kv_self = pltpu.make_async_copy(kvh.at[my_head], kvl.at[far], al)

    def kv_out_loop(i, carry):
        ahead = lax.rem(me + chips + i, devices)
        behind = lax.rem(me + chips - i + devices, devices)
        kv_send(ahead).start()

        @pl.when(i > 0)
        def _():
            kv_send(behind).start()

        return carry

    lax.fori_loop(0, chips, kv_out_loop, 0)
    kv_self.start()
    for k in range(1, chunks):
        q_out(k)

    send_w = remote(wo_hbm, w2.at[c], wos, wor, z, 1 - c)
    send_w.start()
    attf[...] = jnp.zeros_like(attf)
    mf[...] = jnp.zeros_like(mf)
    lf[...] = jnp.zeros_like(lf)

    def kv_in_loop(n, carry):
        @pl.when(n != far)
        def _():
            remote(kvh.at[0], kvl.at[n], as_.at[0], ar.at[n], z, 1 - c).wait_recv()

        return carry

    for load in loads:
        load.wait()

    def a_send(b, k):
        dest = groups * my_head + b
        return remote(ao.at[b, k], a.at[my_group, k], ass.at[b, k], ars.at[my_group, k], dest // 2, lax.rem(dest, 2))

    def a_local(b, k):
        return pltpu.make_async_copy(ao.at[b, k], a.at[my_group, k], als.at[k])

    span = PCAP * per
    contract = (((1,), (1,)), ((), ()))

    def attend(i, carry):
        k, u = i // PAIR, lax.rem(i, PAIR)

        @pl.when(u == 0)
        def _():
            for b in range(groups):
                source = groups * my_head + b

                @pl.when(source != me)
                def _():
                    remote(qs.at[0, 0], ql.at[b, k], qss.at[0, 0], qrs.at[b, k], z, 1 - c).wait_recv()

                @pl.when(source == me)
                def _():
                    q_local(0, k).wait()

            for j in range(per):
                qf[pl.ds(j, CHUNK, stride=per), :] = ql[j // 2, k, :, (j % 2) * HD : (j % 2 + 1) * HD].astype(F32)

        mine = pl.ds(pl.multiple_of(u * span, 8), span)
        qi = qf[mine, :]
        prompt = my_group * per_group + i
        first_row = starts[prompt]
        pscore = lax.dot_general(qi.astype(BF16), pk[i], contract, preferred_element_type=F32) * scaling
        for r in range(PCAP):
            q8 = qf[pl.ds(pl.multiple_of(u * span + r * per, 8), per), :].astype(BF16)
            s8 = lax.dot_general(q8, sk[i * PCAP + r], contract, preferred_element_type=F32) * scaling
            length = lengths[jnp.minimum(first_row + r, rows - 1)]
            seen = lax.broadcasted_iota(jnp.int32, s8.shape, 1) < length
            ss[r * per : (r + 1) * per, :] = jnp.where(seen, s8, -jnp.inf)
        sfx = ss[...]
        top = jnp.maximum(jnp.max(pscore, axis=1, keepdims=True), jnp.max(sfx, axis=1, keepdims=True))
        pe = jnp.exp(pscore - top)
        se = jnp.exp(sfx - top)
        mf[mine, :] = jnp.broadcast_to(top, (span, HD))
        total = jnp.sum(pe, axis=1, keepdims=True) + jnp.sum(se, axis=1, keepdims=True)
        lf[mine, :] = jnp.broadcast_to(total, (span, HD))
        acc = jnp.dot(pe.astype(BF16), pv[i], preferred_element_type=F32)
        ss[...] = se
        for r in range(PCAP):
            w8 = ss[r * per : (r + 1) * per, :].astype(BF16)
            pvacc[r * per : (r + 1) * per, :] = jnp.dot(w8, sv[i * PCAP + r], preferred_element_type=F32)
        attf[mine, :] = acc + pvacc[...]

        @pl.when(i == PAIR - 1)
        def _():
            lax.fori_loop(0, devices, kv_in_loop, 0)
            kv_self.wait()
            table[...] = kvl[...].astype(F32).reshape(rows, 2 * HD).astype(BF16)

        @pl.when(u == PAIR - 1)
        def _():
            pick = select(slot_ids(my_group, k, (CHUNK, rows), 0), 1)
            kv = jnp.dot(pick, table[...], preferred_element_type=F32)
            for j in range(per):
                kf[pl.ds(j, CHUNK, stride=per), :] = kv[:, :HD]
                vf[pl.ds(j, CHUNK, stride=per), :] = kv[:, HD:]
            self_score = jnp.sum(qf[...] * kf[...], axis=1, keepdims=True) * scaling
            peak = jnp.maximum(mf[...], self_score)
            past = jnp.exp(mf[...] - peak)
            own = jnp.exp(self_score - peak)
            attf[...] = (attf[...] * past + own * vf[...]) / (lf[...] * past + own)
            for j in range(per):
                ao[j // 2, k, :, (j % 2) * HD : (j % 2 + 1) * HD] = attf[pl.ds(j, CHUNK, stride=per), :].astype(BF16)
            for b in range(groups):
                dest = groups * my_head + b

                @pl.when(dest != me)
                def _():
                    a_send(b, k).start()

                @pl.when(dest == me)
                def _():
                    a_local(b, k).start()

        return carry

    lax.fori_loop(0, per_group, attend, 0)

    order = lax.broadcasted_iota(jnp.int32, (rows, CHUNK), 0)
    wanted = (lax.rem(order, rows // 2) // 8 * 2 + order // (rows // 2)) * 8 + lax.rem(order, 8)
    picked = jnp.zeros((rows, 2 * HD), F32)
    for k in range(chunks):
        for g in range(groups):
            source = heads * g + me // groups

            @pl.when(source != me)
            def _():
                remote(ao.at[0, 0], a.at[g, k], ass.at[0, 0], ars.at[g, k], z, 1 - c).wait_recv()

            @pl.when(source == me)
            def _():
                a_local(0, k).wait()

            pick = jnp.where(wanted == slot_ids(g, k, (rows, CHUNK), 1), 1.0, 0.0).astype(BF16)
            picked = picked + jnp.dot(pick, a[g, k], preferred_element_type=F32)
    x2[0, 0] = picked[: rows // 2].astype(BF16)
    x2[0, 1] = picked[rows // 2 :].astype(BF16)
    swap = remote(x2.at[0, 1 - c], x2.at[1, 0], xss, xrs, z, 1 - c)
    swap.start()
    send_w.wait()
    rwidth = features // RCH
    ready = 3

    def own_part(j):
        cols = pl.ds(j * rwidth, rwidth)
        p[:, cols] = jnp.dot(x2[0, c], w2[c, :, cols], preferred_element_type=F32).astype(BF16).astype(F32)

    for j in range(ready):
        own_part(j)
    swap.wait()

    def ring(way, step, j):
        return remote(
            rs.at[way, step, j], rr.at[way, step, j], rss.at[way, step, j], rsr.at[way, step, j],
            right if way == 0 else left, c,
        )

    def block_of(chip, cols):
        return p[pl.ds(pl.multiple_of(chip * 8, 8), 8), cols]

    def dest_of(way, s):
        return lax.rem(z + half - s, chips) if way == 0 else lax.rem(z + half + s, chips)

    def starts_far(way, j):
        return (j < RCH // 2) == (way == 0)

    for j in range(RCH):
        if j >= ready:
            own_part(j)
        cols = pl.ds(j * rwidth, rwidth)
        second = jnp.dot(x2[1, 0], w2[1 - c, :, cols], preferred_element_type=F32).astype(BF16).astype(F32)
        p[:, cols] = p[:, cols] + second
        for way in range(2):
            step = 0 if starts_far(way, j) else 1
            rs[way, step, j] = block_of(dest_of(way, step), cols).astype(BF16)
            ring(way, step, j).start()

    def fold_one(way, s, j):
        cols = pl.ds(j * rwidth, rwidth)
        ring(way, s - 1, j).wait_recv()
        rs[way, s, j] = (block_of(dest_of(way, s), cols) + rr[way, s - 1, j].astype(F32)).astype(BF16)
        ring(way, s, j).start()

    for j in range(RCH):
        fold_one(0 if starts_far(0, j) else 1, 1, j)

    def fold(s, carry):
        for j in range(RCH):
            fold_one(0, s, j)
            fold_one(1, s, j)
        return carry

    lax.fori_loop(2, half, fold, 0)
    for j in range(RCH):
        cols = pl.ds(j * rwidth, rwidth)
        ring(0, half - 1, j).wait_recv()
        ring(1, half - 1, j).wait_recv()
        total = block_of(z, cols) + rr[0, half - 1, j].astype(F32) + rr[1, half - 1, j].astype(F32)
        out[:, cols] = (hidden[:, cols].astype(F32) + total).astype(BF16)

    for j in range(XCH):
        row_copy(0, 0, j, me).wait_send()
        row_copy(1, 0, j, me).wait_send()
    part_copy(0, 0, me).wait_send()
    part_copy(0, half, me).wait_send()
    kv_copy(0, 0).wait_send()
    kv_copy(1, 0).wait_send()
    for j in range(RCH):
        ring(0 if starts_far(0, j) else 1, 0, j).wait_send()

    def drain(s, carry):
        for j in range(XCH):

            @pl.when((s < half - 1) | (j < XCH // 2))
            def _():
                row_copy(0, s, j, me).wait_send()

            @pl.when((s < half - 1) | (j >= XCH // 2))
            def _():
                row_copy(1, s, j, me).wait_send()

        part_copy(0, s, me).wait_send()
        part_copy(1, s, me).wait_send()
        kv_copy(0, s).wait_send()
        kv_copy(1, s).wait_send()
        for j in range(RCH):
            ring(0, s, j).wait_send()
            ring(1, s, j).wait_send()

        return carry

    lax.fori_loop(1, half, drain, 0)

    def kv_drain(n, carry):
        @pl.when(n != me)
        def _():
            kv_send(n).wait_send()

        return carry

    lax.fori_loop(0, devices, kv_drain, 0)
    for k in range(chunks):
        for g in range(groups):
            owner = heads * g + z // 2
            dest = groups * my_head + g

            @pl.when(owner != me)
            def _():
                q_send(g, k).wait_send()

            @pl.when(dest != me)
            def _():
                a_send(g, k).wait_send()


def local(
    hidden_in,
    norm_gain,
    w_query,
    w_kv,
    w_out,
    prefix_keys,
    prefix_values,
    suffix_keys,
    suffix_values,
    row_counts,
    suffix_lengths,
):
    chips = lax.axis_size("tensor_0")
    devices = 2 * chips
    own, width = hidden_in.shape
    heads = w_kv.shape[1]
    pair = w_query.shape[1]
    groups = devices // heads
    per_group = row_counts.shape[0] // groups
    chunks = per_group // PAIR
    rows = suffix_lengths.shape[0]
    slab = w_kv.shape[0]
    half = chips // 2
    keys, size = prefix_keys.shape[2], suffix_keys.shape[2]
    columns = heads * 2 * HD
    vmem = pl.BlockSpec(memory_space=pltpu.VMEM)
    smem = pl.BlockSpec(memory_space=pltpu.SMEM)
    anywhere = pl.BlockSpec(memory_space=pl.ANY)
    dma = pltpu.SemaphoreType.DMA

    frequency = 500000.0 ** (-(2.0 * (jnp.arange(HD) % (HD // 2)).astype(F32)) / HD)
    angle = (PREFIX + suffix_lengths).astype(F32)[:, None] * frequency[None, :]
    cosf = jnp.cos(angle)
    sinf = jnp.where(jnp.arange(HD) < HD // 2, -1.0, 1.0)[None, :] * jnp.sin(angle)

    slots = (groups, chunks, CHUNK, pair * HD)
    return pl.pallas_call(
        functools.partial(layer_kernel, chips),
        out_shape=jax.ShapeDtypeStruct((own, width), BF16),
        in_specs=[vmem, vmem] + [anywhere] * 7 + [vmem, vmem, smem, smem],
        out_specs=vmem,
        scratch_shapes=[
            pltpu.VMEM((devices, own, width), BF16),
            pltpu.VMEM((width * pair, HD), BF16),
            pltpu.VMEM((width, pair * HD), BF16),
            pltpu.VMEM((slab * heads * 2, HD), BF16),
            pltpu.VMEM((2 * slab, columns), BF16),
            pltpu.VMEM((PIECE, HD), F32),
            pltpu.VMEM((2, half, own, columns), KVT),
            pltpu.VMEM((2, half, own, columns), KVT),
            pltpu.VMEM(slots, BF16),
            pltpu.VMEM(slots, BF16),
            pltpu.VMEM((heads, own, 2 * HD), BF16),
            pltpu.VMEM((devices, own, 2 * HD), BF16),
            pltpu.VMEM((rows, 2 * HD), BF16),
            pltpu.SMEM((groups * per_group,), jnp.int32),
            pltpu.VMEM((per_group, keys, HD), BF16),
            pltpu.VMEM((per_group, keys, HD), BF16),
            pltpu.VMEM((per_group * PCAP, size, HD), BF16),
            pltpu.VMEM((per_group * PCAP, size, HD), BF16),
            pltpu.VMEM((CHUNK * heads, HD), F32),
            pltpu.VMEM((CHUNK * heads, HD), F32),
            pltpu.VMEM((CHUNK * heads, HD), F32),
            pltpu.VMEM((CHUNK * heads, HD), F32),
            pltpu.VMEM((CHUNK * heads, HD), F32),
            pltpu.VMEM((rows, pair * HD), F32),
            pltpu.VMEM((8 * own, pair * HD), F32),
            pltpu.VMEM((PCAP * heads, size), F32),
            pltpu.VMEM((PCAP * heads, HD), F32),
            pltpu.VMEM((CHUNK * heads, HD), F32),
            pltpu.VMEM(slots, BF16),
            pltpu.VMEM(slots, BF16),
            pltpu.VMEM((2, pair * HD, width), BF16),
            pltpu.VMEM((2, 2, rows // 2, pair * HD), BF16),
            pltpu.VMEM((rows // 2, width), F32),
            pltpu.VMEM((2, half, RCH, own, width // RCH), BF16),
            pltpu.VMEM((2, half, RCH, own, width // RCH), BF16),
            dma, dma, dma, dma, dma, dma, dma, dma((4,)),
            dma((2, half, XCH)), dma((2, half, XCH)),
            dma((2, half + 1)), dma((2, half + 1)),
            dma((2, half)), dma((2, half)),
            dma((groups, chunks)), dma((groups, chunks)), dma((chunks,)),
            dma((devices,)), dma((devices,)), dma,
            dma((groups, chunks)), dma((groups, chunks)), dma((chunks,)),
            dma, dma,
            dma((2, half, RCH)), dma((2, half, RCH)),
        ],
        compiler_params=pltpu.CompilerParams(
            collective_id=0, has_side_effects=True, vmem_limit_bytes=66_000_000
        ),
    )(
        hidden_in,
        norm_gain.reshape(width // HD, HD),
        w_query.reshape(width * pair, HD),
        w_kv.reshape(slab * heads * 2, HD),
        w_out.reshape(pair * HD, width),
        prefix_keys[0],
        prefix_values[0],
        suffix_keys[0],
        suffix_values[0],
        cosf,
        sinf,
        row_counts,
        suffix_lengths,
    )


def solution(mesh):
    cores = 2
    split = Mesh(
        mesh.devices.reshape(mesh.shape["groups"], mesh.shape["tensor"] // cores, cores),
        ("groups", "tensor_0", "tensor_1"),
    )
    return jax.shard_map(
        local,
        mesh=split,
        in_specs=(
            P(GROUPS_TENSOR, None),
            P(),
            P(None, TENSOR, None),
            P(TENSOR, None, None, None),
            P(TENSOR, None, None),
            P(GROUPS_TENSOR, None, None, None),
            P(GROUPS_TENSOR, None, None, None),
            P(GROUPS_TENSOR, None, None, None),
            P(GROUPS_TENSOR, None, None, None),
            P("groups"),
            P("groups"),
        ),
        out_specs=P(GROUPS_TENSOR, None),
        check_vma=False,
    )
```
